32 devices in a mesh: row: 8 (over z, y), col: 4 (over x, core).
Axes of the slice: x: 2, y: 2, z: 4, core: 2. Of those that a mesh axis runs over, the one named last changes fastest.
Arguments:
- moment: bfloat16 [2, 4096, 4096], P(None, 'row', 'col'), may hold values from -6 to 6
- second: float32 [2, 4096, 4096], P(None, 'row', 'col'), may hold values from 0.04 to 2
- left_old: bfloat16 [2, 4096, 4096], P(None, 'col', 'row'), may hold values from -0.09375 to 0.09375
- left_new: bfloat16 [2, 4096, 4096], P(None, 'col', 'row'), may hold values from -0.09375 to 0.09375
- right_old: bfloat16 [4096, 4096], P('row', 'col'), may hold values from -0.09375 to 0.09375
- right_new: bfloat16 [4096, 4096], P('row', 'col'), may hold values from -0.09375 to 0.09375
Outputs:
- moment_new: bfloat16 [2, 4096, 4096], P(None, 'row', 'col')
- direction: bfloat16 [2, 4096, 4096], P(None, 'row', 'col')
The draws below stay inside these ranges and needn't reach their ends.
All inputs are finite; a program needn't handle non-finite values.
Results may differ from the reference program's by a relative error of at most 0.03.
Values may be sent and summed in bfloat16 or wider, within the bound.
A program may use at most 128 MiB of HBM per device.

```python
import math
import jax
import jax.numpy as jnp
from jax import lax

LBLK = 4096
RW = 4096
NBLK = 2
N_ROW = 8
N_COL = 4


def levels(own_key, dims, cuts, low, top_value):
    factor_of = 1.0
    for dim, parts in cuts:
        steps = jax.random.uniform(jax.random.fold_in(jax.random.fold_in(own_key, 6), dim), (parts,), jnp.float32, low / len(cuts), top_value / len(cuts))
        factor_of = factor_of * jnp.repeat(jnp.exp(steps), dims[dim] // parts).reshape((-1,) + (1,) * (len(dims) - 1 - dim))
    return factor_of


def gaussian(stream_key, dims, width, reach, split=(), kind=jnp.bfloat16):
    array = width * jax.random.normal(stream_key, dims, jnp.float32)
    if split:
        array = array * levels(stream_key, dims, split, -0.22, 0.18)
    return jnp.clip(array, -reach, reach).astype(kind)


def setup_inputs(seed: int = 0) -> dict:
    streams_of = jax.random.split(jax.random.key(seed), 7)
    return {
        "moment": gaussian(streams_of[0], (NBLK, LBLK, RW), 1.0, 6.0, ((1, 8), (2, 4))),
        "second": jnp.clip(jnp.exp(math.log(2.0) - 3.912023 * jax.random.uniform(streams_of[1], (NBLK, LBLK, RW), jnp.float32) ** levels(streams_of[1], (NBLK, LBLK, RW), ((1, 8), (2, 4)), -0.2, 0.2)), 0.04, 2.0),
        "left_old": gaussian(streams_of[2], (NBLK, LBLK, LBLK), LBLK ** -0.5, 0.09375, ((1, 4), (2, 8))),
        "left_new": gaussian(streams_of[3], (NBLK, LBLK, LBLK), LBLK ** -0.5, 0.09375, ((1, 4), (2, 8))),
        "right_old": gaussian(streams_of[4], (RW, RW), RW ** -0.5, 0.09375, ((0, 8), (1, 4))),
        "right_new": gaussian(streams_of[5], (RW, RW), RW ** -0.5, 0.09375, ((0, 8), (1, 4))),
    }


def grouped_product(new_basis, old_basis, groups):
    group_rows = new_basis.shape[0] // groups

    def accumulate(running, group_index):
        offset = (group_index * group_rows).astype(jnp.int32)
        new_part = lax.dynamic_slice_in_dim(new_basis, offset, group_rows, 0)
        old_part = lax.dynamic_slice_in_dim(old_basis, offset, group_rows, 0)
        partial_sum = jnp.dot(new_part.T, old_part, preferred_element_type=jnp.float32)
        rounded = lax.optimization_barrier(partial_sum.astype(jnp.bfloat16))
        return (running + rounded.astype(jnp.float32), None)
    start_sum = jnp.zeros((new_basis.shape[1], old_basis.shape[1]), jnp.float32)
    running, unused = lax.scan(accumulate, start_sum, jnp.arange(groups, dtype=jnp.int32))
    return running.astype(jnp.bfloat16)

def reference(moment, second, left_old, left_new, right_old, right_new):
    right_transition = grouped_product(right_new, right_old, N_ROW)

    def one_block(inputs):
        block_moment, block_old, block_new = inputs
        left_transition = grouped_product(block_new, block_old, N_COL)
        rotated = jnp.dot(left_transition, block_moment, preferred_element_type=jnp.float32).astype(jnp.bfloat16)
        return jnp.dot(rotated, right_transition.T, preferred_element_type=jnp.float32).astype(jnp.bfloat16)
    moment_new = lax.map(one_block, (moment, left_old, left_new))
    direction = (moment_new.astype(jnp.float32) / (jnp.sqrt(second) + 1e-08)).astype(jnp.bfloat16)
    return (moment_new, direction)
```

```python
import jax
import jax.numpy as jnp
from jax import lax
from jax.sharding import PartitionSpec as P

F32 = jnp.float32
BF16 = jnp.bfloat16


def add(*terms):
    total = terms[0].astype(F32)
    for term in terms[1:]:
        total = total + term.astype(F32)
    return total.astype(BF16)


class Row:
    def __init__(self, size):
        self.size = size
        self.nz = size // 2
        index = lax.axis_index("row")
        self.z = index // 2
        self.y = index % 2

    def pairs(self, dz, dy, valid):
        out = []
        for z in range(self.nz):
            for y in range(2):
                if valid(z) and 0 <= z + dz < self.nz:
                    out.append((z * 2 + y, (z + dz) * 2 + (y + dy) % 2))
        return out

    def shift(self, value, dz, dy, valid=lambda z: True):
        return lax.ppermute(value, "row", self.pairs(dz, dy, valid))

    def line(self, value):
        right, left = [value], [value]
        for step in range(self.nz - 1):
            right.append(self.shift(right[-1], 1, 0, lambda z: z >= step))
            left.append(self.shift(left[-1], -1, 0, lambda z: z <= self.nz - 1 - step))
        return right[1:], left[1:]

    def slots(self, right, left):
        n = self.nz
        return [jnp.where(self.z > t, right[t], left[n - 2 - t]) for t in range(n - 1)]

    def gather_zy(self, value):
        n = self.nz
        other = self.shift(value, 0, 1)
        right, left = self.line(value)
        across_r = [self.shift(a, 0, 1, lambda z: z > t) for t, a in enumerate(right)]
        across_l = [self.shift(a, 0, 1, lambda z: z < n - 1 - t) for t, a in enumerate(left)]
        mine = self.slots(right, left)
        theirs = self.slots(across_r, across_l)
        return [(value, other)] + list(zip(mine, theirs))

    def gather_yz(self, value):
        other = self.shift(value, 0, 1)
        mine = self.slots(*self.line(value))
        theirs = self.slots(*self.line(other))
        return [(value, other)] + list(zip(mine, theirs))


def exchange(value, size, bit):
    return lax.ppermute(value, "col", [(c, c ^ bit) for c in range(size)])


def sum_over_col(value, size):
    me = lax.axis_index("col")
    bits = [1 << s for s in range(size.bit_length() - 1)]
    for bit in bits:
        half = value.shape[1] // 2
        side = (me // bit) % 2
        sent = lax.dynamic_slice_in_dim(value, (1 - side) * half, half, 1)
        kept = lax.dynamic_slice_in_dim(value, side * half, half, 1)
        value = add(kept, exchange(sent, size, bit))
    for bit in reversed(bits):
        side = (me // bit) % 2
        other = exchange(value, size, bit)
        low = jnp.where(side == 0, value, other)
        high = jnp.where(side == 0, other, value)
        value = jnp.concatenate([low, high], axis=1)
    return value


def gather_col(value, size, axis):
    me = lax.axis_index("col")
    chunks = {0: value}
    for s in reversed(range(size.bit_length() - 1)):
        bit = 1 << s
        for j in list(chunks):
            chunks[j ^ bit] = exchange(chunks[j], size, bit)
    width = value.shape[axis]
    shape = list(value.shape)
    shape[axis] = width * size
    whole = jnp.zeros(shape, value.dtype)
    for j, chunk in chunks.items():
        whole = lax.dynamic_update_slice_in_dim(whole, chunk, (me ^ j) * width, axis)
    return whole


def make_local(n_row, n_col):
    def local(moment, second, left_old, left_new, right_old, right_new):
        row = Row(n_row)
        blocks = moment.shape[0]
        old_slots = row.gather_zy(left_old)
        old_right_rows = lax.all_gather(right_old, "col", axis=1, tiled=True)
        panels = []
        for pair in old_slots:
            terms = [
                jnp.einsum("bwi,bwj->bij", left_new, old, preferred_element_type=F32).astype(BF16)
                for old in pair
            ]
            panels.append(sum_over_col(jnp.concatenate(terms, axis=2), n_col))

        gathers = [
            (row.gather_yz if b < blocks // 2 else row.gather_zy)(moment[b])
            for b in range(blocks)
        ]

        right_terms = jnp.dot(right_new.T, old_right_rows, preferred_element_type=F32)
        right_panel = lax.psum(right_terms.astype(BF16), "row")

        width = moment.shape[1]
        rotated = []
        for b in range(blocks):
            total = None
            for panel, pair in zip(panels, gathers[b]):
                for y, part in enumerate(pair):
                    term = jnp.dot(
                        panel[b, :, y * width:(y + 1) * width], part, preferred_element_type=F32
                    )
                    total = term if total is None else total + term
            rotated.append(gather_col(total.astype(BF16), n_col, 1))

        summed = jnp.einsum("bik,qk->biq", jnp.stack(rotated), right_panel, preferred_element_type=F32)
        moment_new = summed.astype(BF16)
        direction = (moment_new.astype(F32) / (jnp.sqrt(second) + 1e-08)).astype(BF16)
        return (moment_new, direction)

    return local


def solution(mesh):
    return jax.shard_map(
        make_local(mesh.shape["row"], mesh.shape["col"]),
        mesh=mesh,
        in_specs=(
            P(None, "row", "col"),
            P(None, "row", "col"),
            P(None, "col", "row"),
            P(None, "col", "row"),
            P("row", "col"),
            P("row", "col"),
        ),
        out_specs=(P(None, "row", "col"), P(None, "row", "col")),
        check_vma=False,
    )
```
